32 devices in a mesh: blk: 8 (over z, y), chan: 4 (over x, core).
Axes of the slice: x: 2, y: 2, z: 4, core: 2. Of those that a mesh axis runs over, the one named last changes fastest.
Arguments:
- pair_map: int32 [16, 2], P('blk'), may hold values from 0 to 15, as said below
- visibilities: bfloat16 [2, 16, 64, 1024], P(None, 'blk', 'chan'), may hold values from -24 to 24
- model_vis: bfloat16 [2, 16, 64, 1024], P(None, 'blk', 'chan'), may hold values from -7.2 to 7.2
- flag_mask: int32 [16, 64, 1024], P('blk', 'chan'), may hold values 0 or 1
- gain_amp: float32 [512], replicated, may hold values from 0.19 to 3.17
- gain_phase: float32 [512], replicated, may hold values from -3.1416 to 3.1416
- row_index: int32 [4, 8, 8, 256], P('chan', 'blk'), may hold values from -1 to 32767, as said below
- cell_codes: int32 [2, 4, 8, 8, 256], P(None, 'chan', 'blk'), may hold values from 32 to 992
Outputs:
- grid_tiles: float32 [4, 8, 2, 128, 128], P('chan', 'blk')
- solved_gains: float32 [2, 512], replicated
The draws below stay inside these ranges and needn't reach their ends.
Inputs may be any that keep to these rules, and one draw needn't show every extreme that they name: `pair_map`: each row is a pair (p, q) of station blocks with p <= q; no two rows are the same pair; every station block appears in some row. `row_index`: each visibility of an index of blk and a channel group appears in at most one row of that index and group; about half of the rows are -1.
All inputs are finite; a program needn't handle non-finite values. No bound on the sum of `flag_mask` on one device may be relied on, other than what follows from the above.
Results may differ from the reference program's by a relative error of at most 0.009.
Values may be sent and summed in bfloat16 or wider, within the bound.
A program may use at most 64 MiB of HBM per device.

```python
import math
import jax
import jax.numpy as jnp
import numpy as np
from jax import lax

S = 512
BS = 32
PAIRS_DEV = 2
SENDERS = 8
PAIRS = 16
CH_DEV = 16
GROUPS = 4
CHANNELS = 64
ITERS = 3
TS = 128
TILES = 8
CAP = 2
KS = 8
OVER = 8


def pair_table(key):
    block_count = S // BS
    first_np, second_np = np.triu_indices(block_count)
    pair_count = first_np.shape[0]
    shuffled = jax.random.permutation(jax.random.fold_in(key, 101), block_count).astype(jnp.int32)
    half = block_count // 2
    lower_block = jnp.minimum(shuffled[0:2 * half:2], shuffled[1:2 * half:2])
    upper_block = jnp.maximum(shuffled[0:2 * half:2], shuffled[1:2 * half:2])
    covered = lower_block * block_count - lower_block * (lower_block - 1) // 2 + (upper_block - lower_block)
    scores = jax.random.randint(jax.random.fold_in(key, 102), (pair_count,), 0, 1 << 20, dtype=jnp.int32) * 1024
    scores = scores + jnp.arange(pair_count, dtype=jnp.int32)
    scores = scores.at[covered].set(-1 - jnp.arange(half, dtype=jnp.int32))
    chosen = jnp.argsort(scores, stable=True)[:PAIRS]
    first_col = jnp.asarray(first_np, dtype=jnp.int32)[chosen]
    second_col = jnp.asarray(second_np, dtype=jnp.int32)[chosen]
    return jnp.stack((first_col, second_col), axis=1)


def model_values(key):
    full_shape = (2, PAIRS, CHANNELS, BS * BS)
    pattern = jnp.clip(jax.random.normal(jax.random.fold_in(key, 201), full_shape, jnp.float32), -4.0, 4.0)
    spectral = 0.6 + 1.2 * jnp.arange(CHANNELS, dtype=jnp.float32) / max(CHANNELS - 1, 1)
    return pattern * spectral[None, None, :, None]


def station_truth(key):
    amplitude = jax.random.uniform(jax.random.fold_in(key, 301), (S,), jnp.float32, 0.6, 1.4)
    phases = jax.random.uniform(jax.random.fold_in(key, 302), (S,), jnp.float32, -math.pi, math.pi)
    return (amplitude, phases)


def draw_pair_map(key, part):
    return pair_table(key)


def draw_model_vis(key, part):
    return model_values(key).astype(jnp.bfloat16)


def draw_gain_amp(key, part):
    amplitude, phases = station_truth(key)
    lower_scale = jax.random.uniform(jax.random.fold_in(key, 501), (), jnp.float32, 0.55, 0.7)
    upper_scale = jax.random.uniform(jax.random.fold_in(key, 502), (), jnp.float32, 1.4, 1.8)
    picked = jax.random.randint(jax.random.fold_in(key, 503), (), 0, 2, dtype=jnp.int32)
    common = jnp.where(picked == 1, upper_scale, lower_scale)
    jitter = jax.random.uniform(jax.random.fold_in(key, 504), (S,), jnp.float32, 0.9, 1.1)
    return (amplitude * common * jitter).astype(jnp.float32)


def draw_gain_phase(key, part):
    amplitude, phases = station_truth(key)
    common = jax.random.uniform(jax.random.fold_in(key, 505), (), jnp.float32, -math.pi, math.pi)
    jitter = jax.random.uniform(jax.random.fold_in(key, 506), (S,), jnp.float32, -0.3, 0.3)
    angle_sum = phases + common + jitter
    return jnp.arctan2(jnp.sin(angle_sum), jnp.cos(angle_sum)).astype(jnp.float32)


def draw_visibilities(key, part):
    model_full = model_values(key)
    pairs = pair_table(key)
    baseline = jnp.arange(BS * BS, dtype=jnp.int32)
    first_station = pairs[:, 0:1] * BS + baseline[None, :] // BS
    second_station = pairs[:, 1:2] * BS + baseline[None, :] % BS
    amplitude, phases = station_truth(key)
    noise_level = 0.3
    true_real = amplitude * jnp.cos(phases)
    true_imag = amplitude * jnp.sin(phases)
    first_real = true_real[first_station][:, None, :]
    first_imag = true_imag[first_station][:, None, :]
    second_real = true_real[second_station][:, None, :]
    second_imag = true_imag[second_station][:, None, :]
    twisted_real = model_full[0] * second_real + model_full[1] * second_imag
    twisted_imag = model_full[1] * second_real - model_full[0] * second_imag
    noise_terms = jnp.clip(jax.random.normal(jax.random.fold_in(key, 303), model_full.shape, jnp.float32), -4.0, 4.0)
    vis_real = first_real * twisted_real - first_imag * twisted_imag + noise_level * noise_terms[0]
    vis_imag = first_real * twisted_imag + first_imag * twisted_real + noise_level * noise_terms[1]
    return jnp.stack((vis_real, vis_imag)).astype(jnp.bfloat16)


def draw_row_index(key, part):
    visible = PAIRS_DEV * CH_DEV * BS * BS
    row_total = TILES * CAP * 128
    device_keys = jax.random.split(jax.random.fold_in(key, 401), GROUPS * SENDERS)

    def one_device(device_key):
        shuffled = jax.random.permutation(device_key, 2 * visible).astype(jnp.int32)[:row_total]
        return jnp.where(shuffled < visible, shuffled, -1).astype(jnp.int32)
    picked = jax.vmap(one_device)(device_keys)
    return picked.reshape(GROUPS, SENDERS, TILES, CAP * 128)


def touch_ends(result, stream_key, smallest, largest):
    longest = result.shape.index(max(result.shape))
    spots = []
    for shift in (0, 1):
        where = [jax.random.randint(jax.random.fold_in(stream_key, axis), (), 0, length) for axis, length in enumerate(result.shape)]
        where[longest] = (where[longest] + shift) % result.shape[longest]
        spots.append(tuple(where))
    return result.at[spots[0]].set(smallest).at[spots[1]].set(largest)


def setup_inputs(seed: int = 0) -> dict:
    key_of = jax.random.split(jax.random.key(seed), 9)
    return {
        "pair_map": draw_pair_map(jax.random.fold_in(key_of[8], 71), 0),
        "visibilities": draw_visibilities(jax.random.fold_in(key_of[8], 71), 0),
        "model_vis": draw_model_vis(jax.random.fold_in(key_of[8], 71), 0),
        "flag_mask": touch_ends((jax.random.randint(key_of[3], (PAIRS, CHANNELS, BS * BS), 0, 10) < 9).astype(jnp.int32), jax.random.fold_in(key_of[3], 1), 0, 1),
        "gain_amp": draw_gain_amp(jax.random.fold_in(key_of[8], 71), 0),
        "gain_phase": draw_gain_phase(jax.random.fold_in(key_of[8], 71), 0),
        "row_index": draw_row_index(jax.random.fold_in(key_of[8], 71), 0),
        "cell_codes": touch_ends(jax.random.randint(key_of[7], (2, GROUPS, SENDERS, TILES, CAP * 128), (KS // 2) * OVER, (TS - KS // 2) * OVER + 1), jax.random.fold_in(key_of[7], 1), (KS // 2) * OVER, ((TS - KS // 2) * OVER + 1) - 1).astype(jnp.int32),
    }


def kernel_rows(code_values):
    centre = code_values.astype(jnp.float32) / OVER
    cell_axis = jnp.arange(TS, dtype=jnp.float32)
    offset = cell_axis - centre[..., None]
    inside = jnp.abs(offset) < 0.5 * KS
    return jnp.where(inside, jnp.cos(math.pi * offset / KS) ** 2, 0.0).astype(jnp.bfloat16)


def reference(pair_map, visibilities, model_vis, flag_mask, gain_amp, gain_phase, row_index, cell_codes):
    baseline = jnp.arange(BS * BS, dtype=jnp.int32)
    first_station = pair_map[:, 0:1] * BS + baseline[None, :] // BS
    second_station = pair_map[:, 1:2] * BS + baseline[None, :] % BS
    weight = flag_mask.astype(jnp.float32) * (first_station != second_station).astype(jnp.float32)[:, None, :]
    vis_real = visibilities[0].astype(jnp.float32)
    vis_imag = visibilities[1].astype(jnp.float32)
    model_real = model_vis[0].astype(jnp.float32)
    model_imag = model_vis[1].astype(jnp.float32)
    cross_real = weight * (vis_real * model_real + vis_imag * model_imag)
    cross_imag = weight * (vis_imag * model_real - vis_real * model_imag)
    model_power = weight * (model_real * model_real + model_imag * model_imag)
    first_ids = jnp.broadcast_to(first_station[:, None, :], cross_real.shape).reshape(-1)
    second_ids = jnp.broadcast_to(second_station[:, None, :], cross_real.shape).reshape(-1)

    def station_sum(first_term, second_term):
        return (jax.ops.segment_sum(first_term.reshape(-1), first_ids, num_segments=S)
                + jax.ops.segment_sum(second_term.reshape(-1), second_ids, num_segments=S))

    gain_real = gain_amp * jnp.cos(gain_phase)
    gain_imag = gain_amp * jnp.sin(gain_phase)
    for sweep_index in range(ITERS):
        first_real = gain_real[first_station][:, None, :]
        first_imag = gain_imag[first_station][:, None, :]
        second_real = gain_real[second_station][:, None, :]
        second_imag = gain_imag[second_station][:, None, :]
        numerator_real = station_sum(cross_real * second_real - cross_imag * second_imag,
                                     cross_real * first_real + cross_imag * first_imag)
        numerator_imag = station_sum(cross_real * second_imag + cross_imag * second_real,
                                     cross_real * first_imag - cross_imag * first_real)
        denominator = station_sum(model_power * (second_real * second_real + second_imag * second_imag),
                                  model_power * (first_real * first_real + first_imag * first_imag))
        update_real = numerator_real / denominator
        update_imag = numerator_imag / denominator
        if sweep_index % 2 == 1:
            gain_real = 0.5 * (update_real + gain_real)
            gain_imag = 0.5 * (update_imag + gain_imag)
        else:
            gain_real = update_real
            gain_imag = update_imag

    first_real = gain_real[first_station][:, None, :]
    first_imag = gain_imag[first_station][:, None, :]
    second_real = gain_real[second_station][:, None, :]
    second_imag = gain_imag[second_station][:, None, :]
    twisted_real = model_real * second_real + model_imag * second_imag
    twisted_imag = model_imag * second_real - model_real * second_imag
    predicted_real = first_real * twisted_real - first_imag * twisted_imag
    predicted_imag = first_real * twisted_imag + first_imag * twisted_real
    resid_real = (weight * (vis_real - predicted_real)).astype(jnp.bfloat16)
    resid_imag = (weight * (vis_imag - predicted_imag)).astype(jnp.bfloat16)

    def localize(values):
        shaped = values.reshape(SENDERS, PAIRS_DEV, GROUPS, CH_DEV, BS * BS)
        return jnp.transpose(shaped, (2, 0, 1, 3, 4)).reshape(GROUPS, SENDERS, PAIRS_DEV * CH_DEV * BS * BS)

    slot_rows = row_index.reshape(GROUPS, SENDERS, TILES * CAP * 128)
    live_rows = slot_rows >= 0
    safe_rows = jnp.where(live_rows, slot_rows, 0).astype(jnp.int32)

    def pick_rows(values):
        taken = jnp.take_along_axis(localize(values), safe_rows, axis=2)
        return jnp.where(live_rows, taken, 0.0).astype(jnp.bfloat16)

    def by_tile(values):
        shaped = values.reshape(GROUPS, SENDERS, TILES, CAP * 128)
        return jnp.transpose(shaped, (0, 2, 1, 3)).reshape(GROUPS * TILES, SENDERS * CAP * 128)

    rows_real = by_tile(pick_rows(resid_real))
    rows_imag = by_tile(pick_rows(resid_imag))
    codes_u = by_tile(cell_codes[0])
    codes_v = by_tile(cell_codes[1])

    def one_tile(tile_item):
        real_rows, imag_rows, u_values, v_values = tile_item
        kernel_u = kernel_rows(u_values).astype(jnp.float32)
        kernel_v = kernel_rows(v_values).astype(jnp.float32)
        weighted = jnp.stack((kernel_v * real_rows.astype(jnp.float32)[:, None],
                              kernel_v * imag_rows.astype(jnp.float32)[:, None]), axis=1).astype(jnp.bfloat16)
        weighted = lax.optimization_barrier(weighted).astype(jnp.float32)
        return jnp.einsum("rx,rcy->cxy", kernel_u, weighted, precision=lax.Precision.HIGHEST)

    grids = lax.map(one_tile, (rows_real, rows_imag, codes_u, codes_v))
    grid_tiles = grids.reshape(GROUPS, TILES, 2, TS, TS)
    return grid_tiles, jnp.stack((gain_real, gain_imag))
```

```python
import functools
import math

import jax
import jax.numpy as jnp
from jax import lax
from jax.experimental import pallas as pl
from jax.experimental.pallas import tpu as pltpu
from jax.sharding import PartitionSpec as P

ITERS = 3
TS = 128
KS = 8
OVER = 8
LANES = 128
MESH = pl.DeviceIdType.MESH
F32 = jnp.float32
BF16 = jnp.bfloat16


def iota(shape, dim):
    return lax.broadcasted_iota(jnp.int32, shape, dim)


def split3(x):
    hi = x.astype(BF16)
    rest = x - hi.astype(F32)
    mid = rest.astype(BF16)
    low = (rest - mid.astype(F32)).astype(BF16)
    return hi, mid, low


def dot(a, b):
    return jnp.dot(a, b, preferred_element_type=F32)


def loop(count, body, carry):
    if count <= 8:
        for step in range(count):
            carry = body(step, carry)
        return carry
    return lax.fori_loop(0, count, body, carry)


def kernel(
    n_blk,
    n_chan,
    pm_ref,
    vis_ref,
    mod_ref,
    flag_ref,
    amp_ref,
    ph_ref,
    ri_ref,
    cc_ref,
    grid_ref,
    gains_ref,
    rs_src,
    rs_dst,
    ag_src,
    ag_buf,
    data_t,
    row_src,
    row_buf,
    ku_buf,
    kv_buf,
    pa_buf,
    pb_buf,
    ex_a,
    ex_b,
    fold_ab,
    rs_send,
    rs_recv,
    ag_send,
    ag_recv,
    row_send,
    row_recv,
):
    blk = lax.axis_index("blk")
    chan = lax.axis_index("chan")
    n_dev = n_blk * n_chan
    me = blk * n_chan + chan
    slots, n_ch, n_base = vis_ref.shape[1:]
    stations = amp_ref.shape[1]
    side = math.isqrt(n_base)
    quads = stations // LANES
    per = LANES // side
    cuts = n_base // LANES
    halves = cuts // n_chan
    piece = halves * 8
    rows = row_buf.shape[2]
    pairs = slots * n_blk

    def device(step):
        target = lax.rem(me + step, n_dev)
        return (target // n_chan, lax.rem(target, n_chan))

    barrier = pltpu.get_barrier_semaphore()

    def greet(step, carry):
        pl.semaphore_signal(barrier, inc=1, device_id=device(step), device_id_type=MESH)
        return carry

    lax.fori_loop(1, n_dev, greet, 0)

    base = iota((1, n_base), 1)
    same_place = (base // side) == (base % side)
    pm = pm_ref[...]
    sums = []
    masked = [[], [], [], []]
    for slot in range(slots):
        same_block = pm[slot : slot + 1, 0:1] == pm[slot : slot + 1, 1:2]
        keep = jnp.where(jnp.logical_and(same_place, same_block), 0.0, 1.0)
        weight = flag_ref[slot].astype(F32) * keep
        vr = vis_ref[0, slot].astype(F32) * weight
        vi = vis_ref[1, slot].astype(F32) * weight
        mr = mod_ref[0, slot].astype(F32) * weight
        mi = mod_ref[1, slot].astype(F32) * weight
        for held, value in zip(masked, (vr, vi, mr, mi)):
            held.append(value)
        sums.append(
            (
                jnp.sum(vr * mr + vi * mi, axis=0, keepdims=True),
                jnp.sum(vi * mr - vr * mi, axis=0, keepdims=True),
                jnp.sum(mr * mr + mi * mi, axis=0, keepdims=True),
            )
        )
    level = iota((8, n_base), 0)
    stacked = jnp.zeros((8, n_base), F32)
    for comp in range(3):
        for slot in range(slots):
            stacked = jnp.where(level == comp * slots + slot, sums[slot][comp], stacked)
    for c in range(n_chan):
        for half in range(halves):
            cut = (c * halves + half) * LANES
            rs_src[c, half * 8 : half * 8 + 8, :] = stacked[:, cut : cut + LANES]
    tile_rows = slots * n_ch
    for part in range(4):
        full = jnp.concatenate(masked[part], axis=0)
        tall = jnp.concatenate(
            [full[:, cut * LANES : (cut + 1) * LANES] for cut in range(cuts)], axis=0
        )
        data_t[part * LANES : (part + 1) * LANES, :] = tall.T.astype(BF16)

    pl.semaphore_wait(barrier, n_dev - 1)

    rs_copies = []
    for step in range(1, n_chan):
        other = lax.rem(chan + step, n_chan)
        copy = pltpu.make_async_remote_copy(
            src_ref=rs_src.at[other],
            dst_ref=rs_dst.at[step],
            send_sem=rs_send.at[step],
            recv_sem=rs_recv.at[step],
            device_id=(blk, other),
            device_id_type=MESH,
        )
        copy.start()
        rs_copies.append(copy)

    hi_axis = iota((tile_rows * cuts, rows), 0)
    lo_axis = iota((LANES, rows), 0)

    def row_copy(step):
        tile = lax.rem(blk + step, n_blk)
        return pltpu.make_async_remote_copy(
            src_ref=row_src.at[tile],
            dst_ref=row_buf.at[blk],
            send_sem=row_send.at[step],
            recv_sem=row_recv.at[step],
            device_id=(tile, chan),
            device_id_type=MESH,
        )

    def make_rows(tile, out_ref, where):
        place = ri_ref[0, 0, pl.ds(tile, 1), :]
        high = ((place // LANES) % cuts) * tile_rows + place // n_base
        high = jnp.where(place < 0, -1, high)
        low = jnp.where(place < 0, 0, place) % LANES
        pick = jnp.where(hi_axis == high, 1.0, 0.0).astype(BF16)
        got = dot(data_t[...], pick)
        out_ref[where, 0:1, :] = cc_ref[0, 0, 0, pl.ds(tile, 1), :].astype(F32)
        out_ref[where, 1:2, :] = cc_ref[1, 0, 0, pl.ds(tile, 1), :].astype(F32)
        out_ref[where, 2:3, :] = place.astype(F32)
        for part in range(4):
            block = got[part * LANES : (part + 1) * LANES]
            out_ref[where, 3 + part : 4 + part, :] = jnp.sum(
                jnp.where(lo_axis == low, block, 0.0), axis=0, keepdims=True
            )
        out_ref[where, 7:8, :] = jnp.zeros((1, rows), F32)

    def send_rows(step, carry):
        make_rows(lax.rem(blk + step + 1, n_blk), row_src, lax.rem(blk + step + 1, n_blk))
        row_copy(step + 1).start()
        return carry

    loop(n_blk - 1, send_rows, 0)

    for copy in rs_copies:
        copy.wait_recv()
    total = rs_src[chan]
    for step in range(1, n_chan):
        total = total + rs_dst[step]
    sub = iota((piece, LANES), 0)
    for slot in range(slots):
        for which in range(2):
            value = pm[slot : slot + 1, which : which + 1].astype(F32)
            total = jnp.where(sub == slot * 8 + 6 + which, value, total)
    ag_src[...] = total
    own = pl.multiple_of((chan * n_blk + blk) * piece, 8)
    ag_buf[pl.ds(own, piece), :] = total

    def ag_copy(step):
        return pltpu.make_async_remote_copy(
            src_ref=ag_src,
            dst_ref=ag_buf.at[pl.ds(own, piece), :],
            send_sem=ag_send.at[step],
            recv_sem=ag_recv.at[step],
            device_id=device(step),
            device_id_type=MESH,
        )

    def ag_start(step, carry):
        ag_copy(step).start()
        return carry

    lax.fori_loop(1, n_dev, ag_start, 0)

    make_rows(blk, row_buf, blk)

    el = iota((LANES, n_base), 0) % side
    et = iota((LANES, n_base), 1)
    ex_a[...] = jnp.where(el == et // side, 1.0, 0.0).astype(BF16)
    ex_b[...] = jnp.where(el == et % side, 1.0, 0.0).astype(BF16)
    ft = iota((n_base, LANES), 0)
    fl = iota((n_base, LANES), 1) % side
    fold_ab[:, :LANES] = jnp.where(fl == ft // side, 1.0, 0.0).astype(BF16)
    fold_ab[:, LANES:] = jnp.where(fl == ft % side, 1.0, 0.0).astype(BF16)
    amp = amp_ref[...]
    phase = ph_ref[...]
    gain_real = amp * jnp.cos(phase)
    gain_imag = amp * jnp.sin(phase)

    def row_wait(step, carry):
        row_copy(step + 1).wait_recv()
        return carry

    loop(n_blk - 1, row_wait, 0)

    cell = iota((TS, LANES), 0)
    turn = (cell % (2 * KS)).astype(F32) * (math.pi / KS)
    cell_cos = jnp.cos(turn)[:, 0:1]
    cell_sin = jnp.sin(turn)[:, 0:1]
    cell_at = cell[:, 0:1].astype(F32) * OVER
    lane_side = iota((LANES, rows), 0) % side

    def taper(code):
        code_i = code.astype(jnp.int32)
        angle = (code_i % (2 * KS * OVER)).astype(F32) * (math.pi / (KS * OVER))
        wave = cell_cos * jnp.cos(angle) + cell_sin * jnp.sin(angle)
        inside = jnp.abs(cell_at - code) < 0.5 * KS * OVER
        return jnp.where(inside, wave * wave, 0.0).astype(BF16)

    def prepare(k, carry):
        ku_buf[k] = taper(row_buf[k, 0:1, :])
        kv_buf[k] = taper(row_buf[k, 1:2, :])
        place = row_buf[k, 2:3, :].astype(jnp.int32)
        place = jnp.where(place < 0, 0, place)
        pa_buf[k] = jnp.where(lane_side == (place // side) % side, 1.0, 0.0).astype(BF16)
        pb_buf[k] = jnp.where(lane_side == place % side, 1.0, 0.0).astype(BF16)
        return carry

    loop(n_blk, prepare, 0)

    def ag_wait(step, carry):
        ag_copy(step).wait_recv()
        return carry

    lax.fori_loop(1, n_dev, ag_wait, 0)

    def gathered(c, half, row):
        start = c * n_blk * piece + half * 8 + row
        return ag_buf[pl.ds(start, n_blk, stride=piece), :]

    def whole(comp):
        return jnp.concatenate(
            [
                jnp.concatenate(
                    [
                        gathered(c, half, comp * slots + slot)
                        for c in range(n_chan)
                        for half in range(halves)
                    ],
                    axis=1,
                )
                for slot in range(slots)
            ],
            axis=0,
        )

    cross_real, cross_imag, power = whole(0), whole(1), whole(2)
    first = jnp.concatenate([gathered(0, slot, 6) for slot in range(slots)], axis=0)
    second = jnp.concatenate([gathered(0, slot, 7) for slot in range(slots)], axis=0)
    lane_block = iota((pairs, LANES), 1) // side
    mask_a = [first.astype(jnp.int32) == lane_block + per * q for q in range(quads)]
    mask_b = [second.astype(jnp.int32) == lane_block + per * q for q in range(quads)]

    def chosen(gain, mask):
        out = jnp.zeros((pairs, LANES), F32)
        for q in range(quads):
            out = out + jnp.where(mask[q], gain[:, q * LANES : (q + 1) * LANES], 0.0)
        return out

    def pieces(real, imag, mask):
        return jnp.concatenate(split3(chosen(real, mask)) + split3(chosen(imag, mask)), axis=0)

    def joined(x):
        parts = [x[i * pairs : (i + 1) * pairs] for i in range(6)]
        return parts[0] + parts[1] + parts[2], parts[3] + parts[4] + parts[5]

    def placed(first_term, second_term):
        cols = []
        for q in range(quads):
            cols.append(
                jnp.sum(
                    jnp.where(mask_a[q], first_term, 0.0) + jnp.where(mask_b[q], second_term, 0.0),
                    axis=0,
                    keepdims=True,
                )
            )
        return jnp.concatenate(cols, axis=1)

    for sweep in range(ITERS):
        fr, fi = joined(dot(pieces(gain_real, gain_imag, mask_a), ex_a[...]))
        sr, si = joined(dot(pieces(gain_real, gain_imag, mask_b), ex_b[...]))
        terms = jnp.concatenate(
            (
                cross_real * sr - cross_imag * si,
                cross_real * si + cross_imag * sr,
                power * (sr * sr + si * si),
                cross_real * fr + cross_imag * fi,
                cross_real * fi - cross_imag * fr,
                power * (fr * fr + fi * fi),
            ),
            axis=0,
        )
        hi, mid, low = split3(terms)
        folded = dot(hi, fold_ab[...]) + dot(mid, fold_ab[...]) + dot(low, fold_ab[...])
        num_real, num_imag, den = (
            placed(
                folded[c * pairs : (c + 1) * pairs, :LANES],
                folded[(3 + c) * pairs : (4 + c) * pairs, LANES:],
            )
            for c in range(3)
        )
        update_real = num_real / den
        update_imag = num_imag / den
        if sweep % 2 == 1:
            gain_real = 0.5 * (update_real + gain_real)
            gain_imag = 0.5 * (update_imag + gain_imag)
        else:
            gain_real = update_real
            gain_imag = update_imag

    gains_ref[0:1, :] = gain_real
    gains_ref[1:2, :] = gain_imag

    table_a = pieces(gain_real, gain_imag, mask_a)
    table_b = pieces(gain_real, gain_imag, mask_b)
    pair_axis = iota((pairs, rows), 0)

    def grid_rows(k, acc):
        place = row_buf[k, 2:3, :].astype(jnp.int32)
        pair = (jnp.where(place < 0, 0, place) // (n_ch * n_base)) * n_blk + k
        hit = pair_axis == pair

        def pick(x):
            return jnp.sum(jnp.where(hit, x, 0.0), axis=0, keepdims=True)

        ar, ai = (pick(x) for x in joined(dot(table_a, pa_buf[k])))
        br, bi = (pick(x) for x in joined(dot(table_b, pb_buf[k])))
        vr, vi = row_buf[k, 3:4, :], row_buf[k, 4:5, :]
        mr, mi = row_buf[k, 5:6, :], row_buf[k, 6:7, :]
        tr = mr * br + mi * bi
        ti = mi * br - mr * bi
        live = place >= 0
        rr = jnp.where(live, vr - (ar * tr - ai * ti), 0.0).astype(BF16).astype(F32)
        ri = jnp.where(live, vi - (ar * ti + ai * tr), 0.0).astype(BF16).astype(F32)
        kv = kv_buf[k].astype(F32)
        h = jnp.concatenate(((kv * rr).astype(BF16), (kv * ri).astype(BF16)), axis=0)
        return acc + lax.dot_general(
            ku_buf[k], h, (((1,), (1,)), ((), ())), preferred_element_type=F32
        )

    acc = loop(n_blk, grid_rows, jnp.zeros((TS, 2 * TS), F32))
    grid_ref[0, 0, 0] = acc[:, :TS]
    grid_ref[0, 0, 1] = acc[:, TS:]

    for copy in rs_copies:
        copy.wait_send()

    def ag_done(step, carry):
        ag_copy(step).wait_send()
        return carry

    lax.fori_loop(1, n_dev, ag_done, 0)

    def row_done(step, carry):
        row_copy(step + 1).wait_send()
        return carry

    loop(n_blk - 1, row_done, 0)


def shards(
    n_blk, n_chan, pair_map, visibilities, model_vis, flag_mask, gain_amp, gain_phase, row_index, cell_codes
):
    slots, n_ch, n_base = visibilities.shape[1:]
    stations = gain_amp.shape[0]
    rows = row_index.shape[-1]
    n_dev = n_blk * n_chan
    piece = n_base // LANES // n_chan * 8
    dma = pltpu.SemaphoreType.DMA
    return pl.pallas_call(
        functools.partial(kernel, n_blk, n_chan),
        out_shape=(
            jax.ShapeDtypeStruct((1, 1, 2, TS, TS), F32),
            jax.ShapeDtypeStruct((2, stations), F32),
        ),
        in_specs=[pl.BlockSpec(memory_space=pltpu.VMEM)] * 8,
        out_specs=(pl.BlockSpec(memory_space=pltpu.VMEM),) * 2,
        scratch_shapes=[
            pltpu.VMEM((n_chan, piece, LANES), F32),
            pltpu.VMEM((n_chan, piece, LANES), F32),
            pltpu.VMEM((piece, LANES), F32),
            pltpu.VMEM((n_dev * piece, LANES), F32),
            pltpu.VMEM((4 * LANES, slots * n_ch * n_base // LANES), BF16),
            pltpu.VMEM((n_blk, 8, rows), F32),
            pltpu.VMEM((n_blk, 8, rows), F32),
            pltpu.VMEM((n_blk, TS, rows), BF16),
            pltpu.VMEM((n_blk, TS, rows), BF16),
            pltpu.VMEM((n_blk, LANES, rows), BF16),
            pltpu.VMEM((n_blk, LANES, rows), BF16),
            pltpu.VMEM((LANES, n_base), BF16),
            pltpu.VMEM((LANES, n_base), BF16),
            pltpu.VMEM((n_base, 2 * LANES), BF16),
            dma((n_chan,)),
            dma((n_chan,)),
            dma((n_dev,)),
            dma((n_dev,)),
            dma((n_blk,)),
            dma((n_blk,)),
        ],
        compiler_params=pltpu.CompilerParams(
            collective_id=0, has_side_effects=True, vmem_limit_bytes=56 * 1024 * 1024
        ),
        name="solve_and_grid",
    )(
        pair_map,
        visibilities,
        model_vis,
        flag_mask,
        gain_amp.reshape(1, stations),
        gain_phase.reshape(1, stations),
        row_index,
        cell_codes,
    )


def solution(mesh):
    n_blk, n_chan = mesh.shape["blk"], mesh.shape["chan"]
    in_specs = (
        P("blk", None),
        P(None, "blk", "chan", None),
        P(None, "blk", "chan", None),
        P("blk", "chan", None),
        P(),
        P(),
        P("chan", "blk", None, None),
        P(None, "chan", "blk", None, None),
    )
    out_specs = (P("chan", "blk", None, None, None), P())
    return jax.shard_map(
        functools.partial(shards, n_blk, n_chan),
        mesh=mesh,
        in_specs=in_specs,
        out_specs=out_specs,
        check_vma=False,
    )
```

```python
import functools
import math

import jax
import jax.numpy as jnp
from jax import lax
from jax.experimental import pallas as pl
from jax.experimental.pallas import tpu as pltpu
from jax.sharding import PartitionSpec as P

ITERS = 3
TS = 128
KS = 8
OVER = 8
LANES = 128
MESH = pl.DeviceIdType.MESH
F32 = jnp.float32
BF16 = jnp.bfloat16


def iota(shape, dim):
    return lax.broadcasted_iota(jnp.int32, shape, dim)


def split3(x):
    hi = x.astype(BF16)
    rest = x - hi.astype(F32)
    mid = rest.astype(BF16)
    low = (rest - mid.astype(F32)).astype(BF16)
    return hi, mid, low


def dot(a, b):
    return jnp.dot(a, b, preferred_element_type=F32)


def loop(count, body, carry):
    if count <= 8:
        for step in range(count):
            carry = body(step, carry)
        return carry
    return lax.fori_loop(0, count, body, carry)


def kernel(
    n_blk,
    n_chan,
    pm_hbm,
    vis_hbm,
    mod_hbm,
    flag_hbm,
    amp_hbm,
    ph_hbm,
    ri_hbm,
    cc_hbm,
    grid_ref,
    gains_ref,
    pm_ref,
    vis_ref,
    mod_ref,
    flag_ref,
    amp_ref,
    ph_ref,
    ri_ref,
    cc_ref,
    rs_src,
    rs_dst,
    ag_src,
    ag_buf,
    data_t,
    code_src,
    code_buf,
    row_src,
    row_buf,
    ku_buf,
    kv_buf,
    pa_buf,
    pb_buf,
    ex_a,
    ex_b,
    fold_ab,
    rs_send,
    rs_recv,
    ag_send,
    ag_recv,
    code_send,
    code_recv,
    row_send,
    row_recv,
    in_sem,
):
    blk = lax.axis_index("blk")
    chan = lax.axis_index("chan")
    n_dev = n_blk * n_chan
    me = blk * n_chan + chan
    slots, n_ch, n_base = vis_ref.shape[1:]
    stations = amp_ref.shape[1]
    side = math.isqrt(n_base)
    quads = stations // LANES
    per = LANES // side
    cuts = n_base // LANES
    halves = cuts // n_chan
    piece = halves * 8
    rows = row_buf.shape[2]
    pairs = slots * n_blk

    def device(step):
        target = lax.rem(me + step, n_dev)
        return (target // n_chan, lax.rem(target, n_chan))

    loads = [
        pltpu.make_async_copy(src, dst, in_sem.at[i])
        for i, (src, dst) in enumerate(
            (
                (vis_hbm, vis_ref),
                (mod_hbm, mod_ref),
                (flag_hbm, flag_ref),
                (pm_hbm, pm_ref),
                (ri_hbm, ri_ref),
                (cc_hbm, cc_ref),
                (amp_hbm, amp_ref),
                (ph_hbm, ph_ref),
            )
        )
    ]
    for load in loads:
        load.start()
    barrier = pltpu.get_barrier_semaphore()

    def greet(step, carry):
        pl.semaphore_signal(barrier, inc=1, device_id=device(step), device_id_type=MESH)
        return carry

    lax.fori_loop(1, n_dev, greet, 0)

    for load in loads[:4]:
        load.wait()

    base = iota((1, n_base), 1)
    same_place = (base // side) == (base % side)
    pm = pm_ref[...]
    sums = []
    masked = [[], [], [], []]
    for slot in range(slots):
        same_block = pm[slot : slot + 1, 0:1] == pm[slot : slot + 1, 1:2]
        keep = jnp.where(jnp.logical_and(same_place, same_block), 0.0, 1.0)
        weight = flag_ref[slot].astype(F32) * keep
        vr = vis_ref[0, slot].astype(F32) * weight
        vi = vis_ref[1, slot].astype(F32) * weight
        mr = mod_ref[0, slot].astype(F32) * weight
        mi = mod_ref[1, slot].astype(F32) * weight
        for held, value in zip(masked, (vr, vi, mr, mi)):
            held.append(value)
        sums.append(
            (
                jnp.sum(vr * mr + vi * mi, axis=0, keepdims=True),
                jnp.sum(vi * mr - vr * mi, axis=0, keepdims=True),
                jnp.sum(mr * mr + mi * mi, axis=0, keepdims=True),
            )
        )
    level = iota((8, n_base), 0)
    stacked = jnp.zeros((8, n_base), F32)
    for comp in range(3):
        for slot in range(slots):
            stacked = jnp.where(level == comp * slots + slot, sums[slot][comp], stacked)
    for c in range(n_chan):
        for half in range(halves):
            cut = (c * halves + half) * LANES
            rs_src[c, half * 8 : half * 8 + 8, :] = stacked[:, cut : cut + LANES]
    pl.semaphore_wait(barrier, n_dev - 1)

    rs_copies = []
    for step in range(1, n_chan):
        other = lax.rem(chan + step, n_chan)
        copy = pltpu.make_async_remote_copy(
            src_ref=rs_src.at[other],
            dst_ref=rs_dst.at[step],
            send_sem=rs_send.at[step],
            recv_sem=rs_recv.at[step],
            device_id=(blk, other),
            device_id_type=MESH,
        )
        copy.start()
        rs_copies.append(copy)

    for load in loads[4:]:
        load.wait()

    def hand_over(src, dst, send, recv, step):
        tile = lax.rem(blk + step, n_blk)
        return pltpu.make_async_remote_copy(
            src_ref=src.at[tile],
            dst_ref=dst.at[blk],
            send_sem=send.at[step],
            recv_sem=recv.at[step],
            device_id=(tile, chan),
            device_id_type=MESH,
        )

    code_copy = functools.partial(hand_over, code_src, code_buf, code_send, code_recv)
    row_copy = functools.partial(hand_over, row_src, row_buf, row_send, row_recv)

    def make_codes(tile, out_ref, where):
        out_ref[where, 0:1, :] = cc_ref[0, 0, 0, pl.ds(tile, 1), :].astype(F32)
        out_ref[where, 1:2, :] = cc_ref[1, 0, 0, pl.ds(tile, 1), :].astype(F32)
        out_ref[where, 2:3, :] = ri_ref[0, 0, pl.ds(tile, 1), :].astype(F32)
        out_ref[where, 3:8, :] = jnp.zeros((5, rows), F32)

    def send_codes(step, carry):
        tile = lax.rem(blk + step + 1, n_blk)
        make_codes(tile, code_src, tile)
        code_copy(step + 1).start()
        return carry

    loop(n_blk - 1, send_codes, 0)
    make_codes(blk, code_buf, blk)

    tile_rows = slots * n_ch
    for part in range(4):
        full = jnp.concatenate(masked[part], axis=0)
        tall = jnp.concatenate(
            [full[:, cut * LANES : (cut + 1) * LANES] for cut in range(cuts)], axis=0
        )
        data_t[part * LANES : (part + 1) * LANES, :] = tall.T.astype(BF16)

    for copy in rs_copies:
        copy.wait_recv()
    total = rs_src[chan]
    for step in range(1, n_chan):
        total = total + rs_dst[step]
    sub = iota((piece, LANES), 0)
    for slot in range(slots):
        for which in range(2):
            value = pm[slot : slot + 1, which : which + 1].astype(F32)
            total = jnp.where(sub == slot * 8 + 6 + which, value, total)
    ag_src[...] = total
    own = pl.multiple_of((chan * n_blk + blk) * piece, 8)
    ag_buf[pl.ds(own, piece), :] = total

    def ag_copy(step):
        return pltpu.make_async_remote_copy(
            src_ref=ag_src,
            dst_ref=ag_buf.at[pl.ds(own, piece), :],
            send_sem=ag_send.at[step],
            recv_sem=ag_recv.at[step],
            device_id=device(step),
            device_id_type=MESH,
        )

    def ag_start(step, carry):
        ag_copy(step).start()
        return carry

    lax.fori_loop(1, n_dev, ag_start, 0)

    hi_axis = iota((tile_rows * cuts, rows), 0)
    lo_axis = iota((LANES, rows), 0)

    def make_rows(tile, out_ref, where):
        place = ri_ref[0, 0, pl.ds(tile, 1), :]
        high = ((place // LANES) % cuts) * tile_rows + place // n_base
        high = jnp.where(place < 0, -1, high)
        low = jnp.where(place < 0, 0, place) % LANES
        pick = jnp.where(hi_axis == high, 1.0, 0.0).astype(BF16)
        got = dot(data_t[...], pick)
        for part in range(4):
            block = got[part * LANES : (part + 1) * LANES]
            out_ref[where, part : part + 1, :] = jnp.sum(
                jnp.where(lo_axis == low, block, 0.0), axis=0, keepdims=True
            )

    def send_rows(step, carry):
        tile = lax.rem(blk + step + 1, n_blk)
        make_rows(tile, row_src, tile)
        row_copy(step + 1).start()
        return carry

    loop(n_blk - 1, send_rows, 0)
    make_rows(blk, row_buf, blk)

    el = iota((LANES, n_base), 0) % side
    et = iota((LANES, n_base), 1)
    ex_a[...] = jnp.where(el == et // side, 1.0, 0.0).astype(BF16)
    ex_b[...] = jnp.where(el == et % side, 1.0, 0.0).astype(BF16)
    ft = iota((n_base, LANES), 0)
    fl = iota((n_base, LANES), 1) % side
    fold_ab[:, :LANES] = jnp.where(fl == ft // side, 1.0, 0.0).astype(BF16)
    fold_ab[:, LANES:] = jnp.where(fl == ft % side, 1.0, 0.0).astype(BF16)
    amp = amp_ref[...]
    phase = ph_ref[...]
    gain_real = amp * jnp.cos(phase)
    gain_imag = amp * jnp.sin(phase)

    def code_wait(step, carry):
        code_copy(step + 1).wait_recv()
        return carry

    loop(n_blk - 1, code_wait, 0)

    cell = iota((TS, LANES), 0)
    turn = (cell % (2 * KS)).astype(F32) * (math.pi / KS)
    cell_cos = jnp.cos(turn)[:, 0:1]
    cell_sin = jnp.sin(turn)[:, 0:1]
    cell_at = cell[:, 0:1].astype(F32) * OVER
    lane_side = iota((LANES, rows), 0) % side

    def taper(code):
        code_i = code.astype(jnp.int32)
        angle = (code_i % (2 * KS * OVER)).astype(F32) * (math.pi / (KS * OVER))
        wave = cell_cos * jnp.cos(angle) + cell_sin * jnp.sin(angle)
        inside = jnp.abs(cell_at - code) < 0.5 * KS * OVER
        return jnp.where(inside, wave * wave, 0.0).astype(BF16)

    def prepare(k, carry):
        ku_buf[k] = taper(code_buf[k, 0:1, :])
        kv_buf[k] = taper(code_buf[k, 1:2, :])
        place = code_buf[k, 2:3, :].astype(jnp.int32)
        place = jnp.where(place < 0, 0, place)
        pa_buf[k] = jnp.where(lane_side == (place // side) % side, 1.0, 0.0).astype(BF16)
        pb_buf[k] = jnp.where(lane_side == place % side, 1.0, 0.0).astype(BF16)
        return carry

    loop(n_blk, prepare, 0)

    def ag_wait(step, carry):
        ag_copy(step).wait_recv()
        return carry

    lax.fori_loop(1, n_dev, ag_wait, 0)

    def gathered(c, half, row):
        start = c * n_blk * piece + half * 8 + row
        return ag_buf[pl.ds(start, n_blk, stride=piece), :]

    def whole(comp):
        return jnp.concatenate(
            [
                jnp.concatenate(
                    [
                        gathered(c, half, comp * slots + slot)
                        for c in range(n_chan)
                        for half in range(halves)
                    ],
                    axis=1,
                )
                for slot in range(slots)
            ],
            axis=0,
        )

    cross_real, cross_imag, power = whole(0), whole(1), whole(2)
    first = jnp.concatenate([gathered(0, slot, 6) for slot in range(slots)], axis=0)
    second = jnp.concatenate([gathered(0, slot, 7) for slot in range(slots)], axis=0)
    lane_block = iota((pairs, LANES), 1) // side
    mask_a = [first.astype(jnp.int32) == lane_block + per * q for q in range(quads)]
    mask_b = [second.astype(jnp.int32) == lane_block + per * q for q in range(quads)]

    def chosen(gain, mask):
        out = jnp.zeros((pairs, LANES), F32)
        for q in range(quads):
            out = out + jnp.where(mask[q], gain[:, q * LANES : (q + 1) * LANES], 0.0)
        return out

    def pieces(real, imag, mask):
        return jnp.concatenate(split3(chosen(real, mask)) + split3(chosen(imag, mask)), axis=0)

    def joined(x):
        parts = [x[i * pairs : (i + 1) * pairs] for i in range(6)]
        return parts[0] + parts[1] + parts[2], parts[3] + parts[4] + parts[5]

    def placed(first_term, second_term):
        cols = []
        for q in range(quads):
            cols.append(
                jnp.sum(
                    jnp.where(mask_a[q], first_term, 0.0) + jnp.where(mask_b[q], second_term, 0.0),
                    axis=0,
                    keepdims=True,
                )
            )
        return jnp.concatenate(cols, axis=1)

    for sweep in range(ITERS):
        fr, fi = joined(dot(pieces(gain_real, gain_imag, mask_a), ex_a[...]))
        sr, si = joined(dot(pieces(gain_real, gain_imag, mask_b), ex_b[...]))
        terms = jnp.concatenate(
            (
                cross_real * sr - cross_imag * si,
                cross_real * si + cross_imag * sr,
                power * (sr * sr + si * si),
                cross_real * fr + cross_imag * fi,
                cross_real * fi - cross_imag * fr,
                power * (fr * fr + fi * fi),
            ),
            axis=0,
        )
        folded = dot(jnp.concatenate(split3(terms), axis=0), fold_ab[...])
        count = 6 * pairs
        folded = folded[:count] + folded[count : 2 * count] + folded[2 * count :]
        num_real, num_imag, den = (
            placed(
                folded[c * pairs : (c + 1) * pairs, :LANES],
                folded[(3 + c) * pairs : (4 + c) * pairs, LANES:],
            )
            for c in range(3)
        )
        update_real = num_real / den
        update_imag = num_imag / den
        if sweep % 2 == 1:
            gain_real = 0.5 * (update_real + gain_real)
            gain_imag = 0.5 * (update_imag + gain_imag)
        else:
            gain_real = update_real
            gain_imag = update_imag

    gains_ref[0:1, :] = gain_real
    gains_ref[1:2, :] = gain_imag

    table_a = pieces(gain_real, gain_imag, mask_a)
    table_b = pieces(gain_real, gain_imag, mask_b)
    pair_axis = iota((pairs, rows), 0)

    def row_wait(step, carry):
        row_copy(step + 1).wait_recv()
        return carry

    loop(n_blk - 1, row_wait, 0)

    def grid_rows(k, acc):
        place = code_buf[k, 2:3, :].astype(jnp.int32)
        pair = (jnp.where(place < 0, 0, place) // (n_ch * n_base)) * n_blk + k
        hit = pair_axis == pair

        def pick(x):
            return jnp.sum(jnp.where(hit, x, 0.0), axis=0, keepdims=True)

        ar, ai = (pick(x) for x in joined(dot(table_a, pa_buf[k])))
        br, bi = (pick(x) for x in joined(dot(table_b, pb_buf[k])))
        vr, vi = row_buf[k, 0:1, :], row_buf[k, 1:2, :]
        mr, mi = row_buf[k, 2:3, :], row_buf[k, 3:4, :]
        tr = mr * br + mi * bi
        ti = mi * br - mr * bi
        live = place >= 0
        rr = jnp.where(live, vr - (ar * tr - ai * ti), 0.0).astype(BF16).astype(F32)
        ri = jnp.where(live, vi - (ar * ti + ai * tr), 0.0).astype(BF16).astype(F32)
        kv = kv_buf[k].astype(F32)
        h = jnp.concatenate(((kv * rr).astype(BF16), (kv * ri).astype(BF16)), axis=0)
        return acc + lax.dot_general(
            ku_buf[k], h, (((1,), (1,)), ((), ())), preferred_element_type=F32
        )

    acc = loop(n_blk, grid_rows, jnp.zeros((TS, 2 * TS), F32))
    grid_ref[0, 0, 0] = acc[:, :TS]
    grid_ref[0, 0, 1] = acc[:, TS:]

    for copy in rs_copies:
        copy.wait_send()

    def ag_done(step, carry):
        ag_copy(step).wait_send()
        return carry

    lax.fori_loop(1, n_dev, ag_done, 0)

    def row_done(step, carry):
        code_copy(step + 1).wait_send()
        row_copy(step + 1).wait_send()
        return carry

    loop(n_blk - 1, row_done, 0)


def store(grid_in, gains_in, grid_out, gains_out, sem):
    copies = (
        pltpu.make_async_copy(grid_in, grid_out, sem.at[0]),
        pltpu.make_async_copy(gains_in, gains_out, sem.at[1]),
    )
    for copy in copies:
        copy.start()
    for copy in copies:
        copy.wait()


def shards(
    n_blk, n_chan, pair_map, visibilities, model_vis, flag_mask, gain_amp, gain_phase, row_index, cell_codes
):
    slots, n_ch, n_base = visibilities.shape[1:]
    stations = gain_amp.shape[0]
    rows = row_index.shape[-1]
    n_dev = n_blk * n_chan
    piece = n_base // LANES // n_chan * 8
    dma = pltpu.SemaphoreType.DMA
    inputs = (
        pair_map,
        visibilities,
        model_vis,
        flag_mask,
        gain_amp.reshape(1, stations),
        gain_phase.reshape(1, stations),
        row_index,
        cell_codes,
    )
    inputs = tuple(pltpu.with_memory_space_constraint(x, pltpu.HBM) for x in inputs)
    vmem = pl.BlockSpec(memory_space=pltpu.VMEM)
    hbm = pl.BlockSpec(memory_space=pltpu.HBM)
    out_shape = (
        jax.ShapeDtypeStruct((1, 1, 2, TS, TS), F32),
        jax.ShapeDtypeStruct((2, stations), F32),
    )
    results = pl.pallas_call(
        functools.partial(kernel, n_blk, n_chan),
        out_shape=out_shape,
        in_specs=[hbm] * 8,
        out_specs=(vmem, vmem),
        scratch_shapes=[pltpu.VMEM(x.shape, x.dtype) for x in inputs]
        + [
            pltpu.VMEM((n_chan, piece, LANES), F32),
            pltpu.VMEM((n_chan, piece, LANES), F32),
            pltpu.VMEM((piece, LANES), F32),
            pltpu.VMEM((n_dev * piece, LANES), F32),
            pltpu.VMEM((4 * LANES, slots * n_ch * n_base // LANES), BF16),
            pltpu.VMEM((n_blk, 8, rows), F32),
            pltpu.VMEM((n_blk, 8, rows), F32),
            pltpu.VMEM((n_blk, 4, rows), F32),
            pltpu.VMEM((n_blk, 4, rows), F32),
            pltpu.VMEM((n_blk, TS, rows), BF16),
            pltpu.VMEM((n_blk, TS, rows), BF16),
            pltpu.VMEM((n_blk, LANES, rows), BF16),
            pltpu.VMEM((n_blk, LANES, rows), BF16),
            pltpu.VMEM((LANES, n_base), BF16),
            pltpu.VMEM((LANES, n_base), BF16),
            pltpu.VMEM((n_base, 2 * LANES), BF16),
            dma((n_chan,)),
            dma((n_chan,)),
            dma((n_dev,)),
            dma((n_dev,)),
            dma((n_blk,)),
            dma((n_blk,)),
            dma((n_blk,)),
            dma((n_blk,)),
            dma((8,)),
        ],
        compiler_params=pltpu.CompilerParams(
            collective_id=0,
            has_side_effects=True,
            vmem_limit_bytes=(12 + n_blk * 11 // 16) * 1024 * 1024,
        ),
        name="solve_and_grid",
    )(*inputs)
    return pl.pallas_call(
        store,
        out_shape=out_shape,
        in_specs=[vmem] * 2,
        out_specs=(hbm, hbm),
        scratch_shapes=[dma((2,))],
        compiler_params=pltpu.CompilerParams(vmem_limit_bytes=1024 * 1024),
        name="store",
    )(*results)


def solution(mesh):
    n_blk, n_chan = mesh.shape["blk"], mesh.shape["chan"]
    in_specs = (
        P("blk", None),
        P(None, "blk", "chan", None),
        P(None, "blk", "chan", None),
        P("blk", "chan", None),
        P(),
        P(),
        P("chan", "blk", None, None),
        P(None, "chan", "blk", None, None),
    )
    out_specs = (P("chan", "blk", None, None, None), P())
    return jax.shard_map(
        functools.partial(shards, n_blk, n_chan),
        mesh=mesh,
        in_specs=in_specs,
        out_specs=out_specs,
        check_vma=False,
    )
```

```python
import functools
import math

import jax
import jax.numpy as jnp
from jax import lax
from jax.experimental import pallas as pl
from jax.experimental.pallas import tpu as pltpu
from jax.sharding import PartitionSpec as P

ITERS = 3
TS = 128
KS = 8
OVER = 8
LANES = 128
MESH = pl.DeviceIdType.MESH
F32 = jnp.float32
BF16 = jnp.bfloat16


def iota(shape, dim):
    return lax.broadcasted_iota(jnp.int32, shape, dim)


def split3(x):
    hi = x.astype(BF16)
    rest = x - hi.astype(F32)
    mid = rest.astype(BF16)
    low = (rest - mid.astype(F32)).astype(BF16)
    return hi, mid, low


def dot(a, b):
    return jnp.dot(a, b, preferred_element_type=F32)


def loop(count, body, carry):
    if count <= 8:
        for step in range(count):
            carry = body(step, carry)
        return carry
    return lax.fori_loop(0, count, body, carry)


def kernel(
    n_blk,
    n_chan,
    pm_hbm,
    vis_hbm,
    mod_hbm,
    flag_hbm,
    amp_hbm,
    ph_hbm,
    ri_hbm,
    cc_hbm,
    grid_ref,
    gains_ref,
    pm_ref,
    vis_ref,
    mod_ref,
    flag_ref,
    amp_ref,
    ph_ref,
    ri_ref,
    cc_ref,
    rs_src,
    rs_dst,
    ag_src,
    ag_buf,
    data_t,
    code_src,
    code_buf,
    row_src,
    row_buf,
    ku_buf,
    kv_buf,
    pa_buf,
    pb_buf,
    ex_a,
    ex_b,
    fold_ab,
    rs_send,
    rs_recv,
    ag_send,
    ag_recv,
    code_send,
    code_recv,
    row_send,
    row_recv,
    in_sem,
):
    blk = lax.axis_index("blk")
    chan = lax.axis_index("chan")
    n_dev = n_blk * n_chan
    me = blk * n_chan + chan
    slots, n_ch, n_base = vis_ref.shape[1:]
    stations = amp_ref.shape[1]
    side = math.isqrt(n_base)
    quads = stations // LANES
    per = LANES // side
    cuts = n_base // LANES
    halves = cuts // n_chan
    piece = halves * 8
    rows = row_buf.shape[2]
    pairs = slots * n_blk

    def device(step):
        target = lax.rem(me + step, n_dev)
        return (target // n_chan, lax.rem(target, n_chan))

    loads = [
        pltpu.make_async_copy(src, dst, in_sem.at[i])
        for i, (src, dst) in enumerate(
            (
                (vis_hbm, vis_ref),
                (mod_hbm, mod_ref),
                (flag_hbm, flag_ref),
                (pm_hbm, pm_ref),
                (ri_hbm, ri_ref),
                (cc_hbm, cc_ref),
                (amp_hbm, amp_ref),
                (ph_hbm, ph_ref),
            )
        )
    ]
    for load in loads:
        load.start()
    barrier = pltpu.get_barrier_semaphore()

    def greet(step, carry):
        pl.semaphore_signal(barrier, inc=1, device_id=device(step), device_id_type=MESH)
        return carry

    lax.fori_loop(1, n_dev, greet, 0)

    for load in loads[:4]:
        load.wait()

    base = iota((1, n_base), 1)
    same_place = (base // side) == (base % side)
    pm = pm_ref[...]
    sums = []
    masked = [[], [], [], []]
    for slot in range(slots):
        same_block = pm[slot : slot + 1, 0:1] == pm[slot : slot + 1, 1:2]
        keep = jnp.where(jnp.logical_and(same_place, same_block), 0.0, 1.0)
        weight = flag_ref[slot].astype(F32) * keep
        vr = vis_ref[0, slot].astype(F32) * weight
        vi = vis_ref[1, slot].astype(F32) * weight
        mr = mod_ref[0, slot].astype(F32) * weight
        mi = mod_ref[1, slot].astype(F32) * weight
        for held, value in zip(masked, (vr, vi, mr, mi)):
            held.append(value)
        sums.append(
            (
                jnp.sum(vr * mr + vi * mi, axis=0, keepdims=True),
                jnp.sum(vi * mr - vr * mi, axis=0, keepdims=True),
                jnp.sum(mr * mr + mi * mi, axis=0, keepdims=True),
            )
        )
    level = iota((8, n_base), 0)
    stacked = jnp.zeros((8, n_base), F32)
    for comp in range(3):
        for slot in range(slots):
            stacked = jnp.where(level == comp * slots + slot, sums[slot][comp], stacked)
    for c in range(n_chan):
        for half in range(halves):
            cut = (c * halves + half) * LANES
            rs_src[c, half * 8 : half * 8 + 8, :] = stacked[:, cut : cut + LANES]
    pl.semaphore_wait(barrier, n_dev - 1)

    rs_copies = []
    for step in range(1, n_chan):
        other = lax.rem(chan + step, n_chan)
        copy = pltpu.make_async_remote_copy(
            src_ref=rs_src.at[other],
            dst_ref=rs_dst.at[step],
            send_sem=rs_send.at[step],
            recv_sem=rs_recv.at[step],
            device_id=(blk, other),
            device_id_type=MESH,
        )
        copy.start()
        rs_copies.append(copy)

    for load in loads[4:]:
        load.wait()

    def hand_over(src, dst, send, recv, step):
        tile = lax.rem(blk + step, n_blk)
        return pltpu.make_async_remote_copy(
            src_ref=src.at[tile],
            dst_ref=dst.at[blk],
            send_sem=send.at[step],
            recv_sem=recv.at[step],
            device_id=(tile, chan),
            device_id_type=MESH,
        )

    code_copy = functools.partial(hand_over, code_src, code_buf, code_send, code_recv)
    row_copy = functools.partial(hand_over, row_src, row_buf, row_send, row_recv)

    def make_codes(tile, out_ref, where):
        out_ref[where, 0:1, :] = cc_ref[0, 0, 0, pl.ds(tile, 1), :].astype(F32)
        out_ref[where, 1:2, :] = cc_ref[1, 0, 0, pl.ds(tile, 1), :].astype(F32)
        out_ref[where, 2:3, :] = ri_ref[0, 0, pl.ds(tile, 1), :].astype(F32)
        out_ref[where, 3:8, :] = jnp.zeros((5, rows), F32)

    def send_codes(step, carry):
        tile = lax.rem(blk + step + 1, n_blk)
        make_codes(tile, code_src, tile)
        code_copy(step + 1).start()
        return carry

    loop(n_blk - 1, send_codes, 0)
    make_codes(blk, code_buf, blk)

    tile_rows = slots * n_ch
    for part in range(4):
        full = jnp.concatenate(masked[part], axis=0)
        tall = jnp.concatenate(
            [full[:, cut * LANES : (cut + 1) * LANES] for cut in range(cuts)], axis=0
        )
        data_t[part * LANES : (part + 1) * LANES, :] = tall.T.astype(BF16)

    hi_axis = iota((tile_rows * cuts, rows), 0)
    lo_axis = iota((LANES, rows), 0)

    def make_rows(tile, out_ref, where):
        place = ri_ref[0, 0, pl.ds(tile, 1), :]
        high = ((place // LANES) % cuts) * tile_rows + place // n_base
        high = jnp.where(place < 0, -1, high)
        low = jnp.where(place < 0, 0, place) % LANES
        pick = jnp.where(hi_axis == high, 1.0, 0.0).astype(BF16)
        got = dot(data_t[...], pick)
        for part in range(4):
            block = got[part * LANES : (part + 1) * LANES]
            out_ref[where, part : part + 1, :] = jnp.sum(
                jnp.where(lo_axis == low, block, 0.0), axis=0, keepdims=True
            )

    def send_rows(step, carry):
        tile = lax.rem(blk + step + 1, n_blk)
        make_rows(tile, row_src, tile)
        row_copy(step + 1).start()
        return carry

    loop(n_blk - 1, send_rows, 0)

    for copy in rs_copies:
        copy.wait_recv()
    total = rs_src[chan]
    for step in range(1, n_chan):
        total = total + rs_dst[step]
    sub = iota((piece, LANES), 0)
    for slot in range(slots):
        for which in range(2):
            value = pm[slot : slot + 1, which : which + 1].astype(F32)
            total = jnp.where(sub == slot * 8 + 6 + which, value, total)
    ag_src[...] = total
    own = pl.multiple_of((chan * n_blk + blk) * piece, 8)
    ag_buf[pl.ds(own, piece), :] = total

    def ag_copy(step):
        return pltpu.make_async_remote_copy(
            src_ref=ag_src,
            dst_ref=ag_buf.at[pl.ds(own, piece), :],
            send_sem=ag_send.at[step],
            recv_sem=ag_recv.at[step],
            device_id=device(step),
            device_id_type=MESH,
        )

    def ag_start(step, carry):
        ag_copy(step).start()
        return carry

    lax.fori_loop(1, n_dev, ag_start, 0)

    make_rows(blk, row_buf, blk)
    el = iota((LANES, n_base), 0) % side
    et = iota((LANES, n_base), 1)
    ex_a[...] = jnp.where(el == et // side, 1.0, 0.0).astype(BF16)
    ex_b[...] = jnp.where(el == et % side, 1.0, 0.0).astype(BF16)
    ft = iota((n_base, LANES), 0)
    fl = iota((n_base, LANES), 1) % side
    fold_ab[:, :LANES] = jnp.where(fl == ft // side, 1.0, 0.0).astype(BF16)
    fold_ab[:, LANES:] = jnp.where(fl == ft % side, 1.0, 0.0).astype(BF16)
    amp = amp_ref[...]
    phase = ph_ref[...]
    gain_real = amp * jnp.cos(phase)
    gain_imag = amp * jnp.sin(phase)

    def code_wait(step, carry):
        code_copy(step + 1).wait_recv()
        return carry

    loop(n_blk - 1, code_wait, 0)

    cell = iota((TS, LANES), 0)
    turn = (cell % (2 * KS)).astype(F32) * (math.pi / KS)
    cell_cos = jnp.cos(turn)[:, 0:1]
    cell_sin = jnp.sin(turn)[:, 0:1]
    cell_at = cell[:, 0:1].astype(F32) * OVER
    lane_side = iota((LANES, rows), 0) % side

    def taper(code):
        code_i = code.astype(jnp.int32)
        angle = (code_i % (2 * KS * OVER)).astype(F32) * (math.pi / (KS * OVER))
        wave = cell_cos * jnp.cos(angle) + cell_sin * jnp.sin(angle)
        inside = jnp.abs(cell_at - code) < 0.5 * KS * OVER
        return jnp.where(inside, wave * wave, 0.0).astype(BF16)

    def prepare(k, carry):
        ku_buf[k] = taper(code_buf[k, 0:1, :])
        kv_buf[k] = taper(code_buf[k, 1:2, :])
        place = code_buf[k, 2:3, :].astype(jnp.int32)
        place = jnp.where(place < 0, 0, place)
        pa_buf[k] = jnp.where(lane_side == (place // side) % side, 1.0, 0.0).astype(BF16)
        pb_buf[k] = jnp.where(lane_side == place % side, 1.0, 0.0).astype(BF16)
        return carry

    loop(n_blk, prepare, 0)

    def ag_wait(step, carry):
        ag_copy(step).wait_recv()
        return carry

    lax.fori_loop(1, n_dev, ag_wait, 0)

    def gathered(c, half, row):
        start = c * n_blk * piece + half * 8 + row
        return ag_buf[pl.ds(start, n_blk, stride=piece), :]

    def whole(comp):
        return jnp.concatenate(
            [
                jnp.concatenate(
                    [
                        gathered(c, half, comp * slots + slot)
                        for c in range(n_chan)
                        for half in range(halves)
                    ],
                    axis=1,
                )
                for slot in range(slots)
            ],
            axis=0,
        )

    cross_real, cross_imag, power = whole(0), whole(1), whole(2)
    first = jnp.concatenate([gathered(0, slot, 6) for slot in range(slots)], axis=0)
    second = jnp.concatenate([gathered(0, slot, 7) for slot in range(slots)], axis=0)
    lane_block = iota((pairs, LANES), 1) // side
    mask_a = [first.astype(jnp.int32) == lane_block + per * q for q in range(quads)]
    mask_b = [second.astype(jnp.int32) == lane_block + per * q for q in range(quads)]

    def chosen(gain, mask):
        out = jnp.zeros((pairs, LANES), F32)
        for q in range(quads):
            out = out + jnp.where(mask[q], gain[:, q * LANES : (q + 1) * LANES], 0.0)
        return out

    def pieces(real, imag, mask):
        return jnp.concatenate(split3(chosen(real, mask)) + split3(chosen(imag, mask)), axis=0)

    def joined(x):
        parts = [x[i * pairs : (i + 1) * pairs] for i in range(6)]
        return parts[0] + parts[1] + parts[2], parts[3] + parts[4] + parts[5]

    def placed(first_term, second_term):
        cols = []
        for q in range(quads):
            cols.append(
                jnp.sum(
                    jnp.where(mask_a[q], first_term, 0.0) + jnp.where(mask_b[q], second_term, 0.0),
                    axis=0,
                    keepdims=True,
                )
            )
        return jnp.concatenate(cols, axis=1)

    for sweep in range(ITERS):
        fr, fi = joined(dot(pieces(gain_real, gain_imag, mask_a), ex_a[...]))
        sr, si = joined(dot(pieces(gain_real, gain_imag, mask_b), ex_b[...]))
        terms = jnp.concatenate(
            (
                cross_real * sr - cross_imag * si,
                cross_real * si + cross_imag * sr,
                power * (sr * sr + si * si),
                cross_real * fr + cross_imag * fi,
                cross_real * fi - cross_imag * fr,
                power * (fr * fr + fi * fi),
            ),
            axis=0,
        )
        folded = dot(jnp.concatenate(split3(terms)[:2], axis=0), fold_ab[...])
        count = 6 * pairs
        folded = folded[:count] + folded[count : 2 * count]
        num_real, num_imag, den = (
            placed(
                folded[c * pairs : (c + 1) * pairs, :LANES],
                folded[(3 + c) * pairs : (4 + c) * pairs, LANES:],
            )
            for c in range(3)
        )
        update_real = num_real / den
        update_imag = num_imag / den
        if sweep % 2 == 1:
            gain_real = 0.5 * (update_real + gain_real)
            gain_imag = 0.5 * (update_imag + gain_imag)
        else:
            gain_real = update_real
            gain_imag = update_imag

    gains_ref[0:1, :] = gain_real
    gains_ref[1:2, :] = gain_imag

    table_a = pieces(gain_real, gain_imag, mask_a)
    table_b = pieces(gain_real, gain_imag, mask_b)
    pair_axis = iota((pairs, rows), 0)

    def row_wait(step, carry):
        row_copy(step + 1).wait_recv()
        return carry

    loop(n_blk - 1, row_wait, 0)

    def grid_rows(k, acc):
        place = code_buf[k, 2:3, :].astype(jnp.int32)
        pair = (jnp.where(place < 0, 0, place) // (n_ch * n_base)) * n_blk + k
        hit = pair_axis == pair

        def pick(x):
            return jnp.sum(jnp.where(hit, x, 0.0), axis=0, keepdims=True)

        ar, ai = (pick(x) for x in joined(dot(table_a, pa_buf[k])))
        br, bi = (pick(x) for x in joined(dot(table_b, pb_buf[k])))
        vr, vi = row_buf[k, 0:1, :], row_buf[k, 1:2, :]
        mr, mi = row_buf[k, 2:3, :], row_buf[k, 3:4, :]
        tr = mr * br + mi * bi
        ti = mi * br - mr * bi
        live = place >= 0
        rr = jnp.where(live, vr - (ar * tr - ai * ti), 0.0).astype(BF16).astype(F32)
        ri = jnp.where(live, vi - (ar * ti + ai * tr), 0.0).astype(BF16).astype(F32)
        kv = kv_buf[k].astype(F32)
        h = jnp.concatenate(((kv * rr).astype(BF16), (kv * ri).astype(BF16)), axis=0)
        return acc + lax.dot_general(
            ku_buf[k], h, (((1,), (1,)), ((), ())), preferred_element_type=F32
        )

    acc = loop(n_blk, grid_rows, jnp.zeros((TS, 2 * TS), F32))
    grid_ref[0, 0, 0] = acc[:, :TS]
    grid_ref[0, 0, 1] = acc[:, TS:]

    for copy in rs_copies:
        copy.wait_send()

    def ag_done(step, carry):
        ag_copy(step).wait_send()
        return carry

    lax.fori_loop(1, n_dev, ag_done, 0)

    def row_done(step, carry):
        code_copy(step + 1).wait_send()
        row_copy(step + 1).wait_send()
        return carry

    loop(n_blk - 1, row_done, 0)


def store(grid_in, gains_in, grid_out, gains_out, sem):
    copies = (
        pltpu.make_async_copy(grid_in, grid_out, sem.at[0]),
        pltpu.make_async_copy(gains_in, gains_out, sem.at[1]),
    )
    for copy in copies:
        copy.start()
    for copy in copies:
        copy.wait()


def shards(
    n_blk, n_chan, pair_map, visibilities, model_vis, flag_mask, gain_amp, gain_phase, row_index, cell_codes
):
    slots, n_ch, n_base = visibilities.shape[1:]
    stations = gain_amp.shape[0]
    rows = row_index.shape[-1]
    n_dev = n_blk * n_chan
    piece = n_base // LANES // n_chan * 8
    dma = pltpu.SemaphoreType.DMA
    inputs = (
        pair_map,
        visibilities,
        model_vis,
        flag_mask,
        gain_amp.reshape(1, stations),
        gain_phase.reshape(1, stations),
        row_index,
        cell_codes,
    )
    inputs = tuple(pltpu.with_memory_space_constraint(x, pltpu.HBM) for x in inputs)
    vmem = pl.BlockSpec(memory_space=pltpu.VMEM)
    hbm = pl.BlockSpec(memory_space=pltpu.HBM)
    out_shape = (
        jax.ShapeDtypeStruct((1, 1, 2, TS, TS), F32),
        jax.ShapeDtypeStruct((2, stations), F32),
    )
    results = pl.pallas_call(
        functools.partial(kernel, n_blk, n_chan),
        out_shape=out_shape,
        in_specs=[hbm] * 8,
        out_specs=(vmem, vmem),
        scratch_shapes=[pltpu.VMEM(x.shape, x.dtype) for x in inputs]
        + [
            pltpu.VMEM((n_chan, piece, LANES), F32),
            pltpu.VMEM((n_chan, piece, LANES), F32),
            pltpu.VMEM((piece, LANES), F32),
            pltpu.VMEM((n_dev * piece, LANES), F32),
            pltpu.VMEM((4 * LANES, slots * n_ch * n_base // LANES), BF16),
            pltpu.VMEM((n_blk, 8, rows), F32),
            pltpu.VMEM((n_blk, 8, rows), F32),
            pltpu.VMEM((n_blk, 4, rows), F32),
            pltpu.VMEM((n_blk, 4, rows), F32),
            pltpu.VMEM((n_blk, TS, rows), BF16),
            pltpu.VMEM((n_blk, TS, rows), BF16),
            pltpu.VMEM((n_blk, LANES, rows), BF16),
            pltpu.VMEM((n_blk, LANES, rows), BF16),
            pltpu.VMEM((LANES, n_base), BF16),
            pltpu.VMEM((LANES, n_base), BF16),
            pltpu.VMEM((n_base, 2 * LANES), BF16),
            dma((n_chan,)),
            dma((n_chan,)),
            dma((n_dev,)),
            dma((n_dev,)),
            dma((n_blk,)),
            dma((n_blk,)),
            dma((n_blk,)),
            dma((n_blk,)),
            dma((8,)),
        ],
        compiler_params=pltpu.CompilerParams(
            collective_id=0,
            has_side_effects=True,
            vmem_limit_bytes=(12 + n_blk * 11 // 16) * 1024 * 1024,
        ),
        name="solve_and_grid",
    )(*inputs)
    return pl.pallas_call(
        store,
        out_shape=out_shape,
        in_specs=[vmem] * 2,
        out_specs=(hbm, hbm),
        scratch_shapes=[dma((2,))],
        compiler_params=pltpu.CompilerParams(vmem_limit_bytes=1024 * 1024),
        name="store",
    )(*results)


def solution(mesh):
    n_blk, n_chan = mesh.shape["blk"], mesh.shape["chan"]
    in_specs = (
        P("blk", None),
        P(None, "blk", "chan", None),
        P(None, "blk", "chan", None),
        P("blk", "chan", None),
        P(),
        P(),
        P("chan", "blk", None, None),
        P(None, "chan", "blk", None, None),
    )
    out_specs = (P("chan", "blk", None, None, None), P())
    return jax.shard_map(
        functools.partial(shards, n_blk, n_chan),
        mesh=mesh,
        in_specs=in_specs,
        out_specs=out_specs,
        check_vma=False,
    )
```
